512 devices in a mesh: row: 32 (over y_lo, x, core), col: 16 (over z, y_hi).
Axes of the slice: x: 4, y: 8 (y_hi: 2, y_lo: 4; y = y_hi * 4 + y_lo), z: 8, core: 2. Of those that a mesh axis runs over, the one named last changes fastest.
Arguments:
- left_act: bfloat16 [32, 64, 1024], P(None, 'col', 'row'), may hold values from -6 to 6
- right_act: bfloat16 [32, 64, 1024], P(None, 'row', 'col'), may hold values from -6 to 6
- cotangent: bfloat16 [1024, 1024, 128], P('row', 'col'), may hold values from -4 to 4
- weight: bfloat16 [1024, 128], replicated, may hold values from -0.1875 to 0.1875
Outputs:
- grad_left: float32 [32, 64, 1024], P(None, 'col', 'row')
- grad_right: float32 [32, 64, 1024], P(None, 'row', 'col')
- grad_weight: float32 [1024, 128], P('row')
The draws below stay inside these ranges and needn't reach their ends.
All inputs are finite; a program needn't handle non-finite values.
Results may differ from the reference program's by a relative error of at most 0.0029.
Values may be sent and summed in bfloat16 or wider, within the bound.
A program may use at most 128 MiB of HBM per device.

```python
import jax
import jax.numpy as jnp
from jax import lax

C = 32
E = 128
S = 64
TI = 32
TOKENS = 1024


def levels(own_key, shape, cuts, least, high):
    def one(position, shards_of):
        steps = jax.random.uniform(jax.random.fold_in(jax.random.fold_in(own_key, 6), position), (shards_of,), jnp.float32, least / len(cuts), high / len(cuts))
        return jnp.repeat(jnp.exp(steps), shape[position] // shards_of).reshape((-1,) + (1,) * (len(shape) - position - 1))

    gain = one(*cuts[0])
    for cut in cuts[1:]:
        gain = gain * one(*cut)
    return gain


def centred(key, dims, deviation, most, shards=(), kind=jnp.bfloat16):
    array = jax.random.normal(key, dims, jnp.float32) * deviation
    if len(shards) > 0:
        array = levels(key, dims, shards, -0.22, 0.18) * array
    return jnp.clip(array, min=-most, max=most).astype(kind)


def setup_inputs(seed: int = 0) -> dict:
    key_list = jax.random.split(jax.random.key(seed), 5)
    return {
        "left_act": centred(key_list[0], (C, S, TOKENS), 1.0, 6.0, ((1, 16), (2, 32))),
        "right_act": centred(key_list[1], (C, S, TOKENS), 1.0, 6.0, ((1, 32), (2, 16))),
        "cotangent": centred(key_list[2], (TOKENS, TOKENS, E), 0.5, 4.0, ((0, 32), (1, 16))),
        "weight": centred(key_list[3], (C * C, E), (C * C) ** -0.5, 0.1875),
    }


def reference(left_act, right_act, cotangent, weight):
    blocks = TOKENS // TI
    left = left_act.astype(jnp.float32).reshape(C, S, blocks, TI).transpose(2, 0, 1, 3)
    grads = cotangent.reshape(blocks, TI, TOKENS, E)
    right = right_act.astype(jnp.float32)

    def step(carry, item):
        grad_w, grad_r = carry
        left_blk, grad_blk = item
        outer = (jnp.einsum('csi,dsj->ijcd', left_blk, right) / S).astype(jnp.bfloat16)
        outer_flat = outer.reshape(TI * TOKENS, C * C)
        grad_flat = grad_blk.reshape(TI * TOKENS, E)
        grad_w = grad_w + jnp.dot(outer_flat.T, grad_flat, preferred_element_type=jnp.float32)
        grad_outer = jnp.dot(grad_flat, weight.T, preferred_element_type=jnp.float32).astype(jnp.bfloat16)
        grad_outer = grad_outer.reshape(TI, TOKENS, C, C).astype(jnp.float32)
        grad_l = jnp.einsum('ijcd,dsj->csi', grad_outer, right) / S
        grad_r = grad_r + jnp.einsum('ijcd,csi->dsj', grad_outer, left_blk) / S
        return (grad_w, grad_r), grad_l

    start = (jnp.zeros((C * C, E), jnp.float32), jnp.zeros((C, S, TOKENS), jnp.float32))
    (grad_weight, grad_right), pieces = lax.scan(step, start, (left, grads))
    grad_left = pieces.transpose(1, 2, 0, 3).reshape(C, S, TOKENS)
    return grad_left, grad_right, grad_weight
```

```python
import jax
import jax.numpy as jnp
from jax import lax
from jax.experimental import pallas as pl
from jax.experimental.pallas import tpu as pltpu
from jax.sharding import PartitionSpec as P

BF = jnp.bfloat16
F32 = jnp.float32
MESH = pl.DeviceIdType.MESH
S = 64
C = 32
Q = 16
Z = 8


def dot(a, b, dims=((1,), (0,))):
    return lax.dot_general(a, b, (dims, ((), ())), preferred_element_type=F32)


def kernel(
    rmsg, lmsg, g, w,
    gl_out, gr_out, gw_out,
    rbuf, lbuf, fr, fl, wf, wp, lt, l2, bd, xb, yb,
    gws, gwp, gwh, gwsend, gwrecv, gwz, gwzs, gwy, gwys,
    grs, grp, grh, grsend, grrecv,
    gls, glsend, glrecv, gly, glys,
    rs, rr, ls, lf, lr, pair_s, pair_r, ws, wr, gs, gr, zws, zwr, zls, zlr, ys, yr,
):
    row, col = lax.axis_index("row"), lax.axis_index("col")
    core, q = lax.rem(row, 2), row // 2
    yh, z = lax.rem(col, 2), col // 2
    pair = (row + 1 - 2 * core, col)
    other = (row, col + 1 - 2 * yh)

    def chip(k):
        return lax.rem(q + k, Q)

    def level(k):
        return lax.rem(z + k, Z)

    def row_mate(k):
        return (2 * chip(k) + core, col)

    def z_mate(k):
        return (row, 2 * level(k) + yh)

    def remote(src, dst, send, recv, device):
        return pltpu.make_async_remote_copy(
            src_ref=src, dst_ref=dst, send_sem=send, recv_sem=recv,
            device_id=device, device_id_type=MESH,
        )

    def each(first, last, step):
        def body(k, carry):
            step(k)
            return carry

        lax.fori_loop(first, last, body, 0)

    barrier = pltpu.get_barrier_semaphore()

    def greet(device):
        pl.semaphore_signal(barrier, inc=1, device_id=device, device_id_type=MESH)

    greet(pair)
    greet(other)
    each(1, Q, lambda k: greet(row_mate(k)))
    each(1, Z, lambda k: greet(z_mate(k)))

    wf[...] = w[...].astype(F32)

    def order_weight(d):
        for half in range(2):
            rows = wf[pl.ds(half * C + d, Q, stride=2 * C), :]
            wp[pl.ds(pl.multiple_of(d * C + half * Q, Q), Q), :] = rows.astype(BF)

    each(0, C, order_weight)
    rbuf[core, q] = rmsg[...]
    lbuf[col] = lmsg[...]

    pl.semaphore_wait(barrier, Q + Z)

    def r_copy(k, slot):
        return remote(rmsg, rbuf.at[core, slot], rs.at[k], rr.at[slot], row_mate(k))

    def l_copy(k, slot):
        return remote(lmsg, lbuf.at[slot], ls.at[k], lr.at[slot], z_mate(k))

    def l_side(slot):
        return remote(lmsg, lbuf.at[slot], ls.at[0], lr.at[slot], other)

    l_side(col).start()
    each(1, Q, lambda k: r_copy(k, q).start())
    each(1, Z, lambda k: l_copy(k, col).start())

    def grad_outer(p):
        gp = g[pl.ds(pl.multiple_of(p * 256, 256), 256), :]
        y = dot(wp[...], gp, ((1,), (1,))).astype(BF)
        yb[2 * p] = y[:, :128].reshape(C, C, 128)
        yb[2 * p + 1] = y[:, 128:].reshape(C, C, 128)

    each(0, 8, grad_outer)

    side_col = col + 1 - 2 * yh
    l_side(side_col).wait_recv()

    def l_forward(k, slot):
        return remote(lbuf.at[slot], lbuf.at[slot], lf.at[k], lr.at[slot], z_mate(k))

    each(1, Z, lambda k: l_forward(k, side_col).start())

    each(1, Q, lambda k: r_copy(k, chip(k)).wait_recv())

    def r_pair(half):
        return remote(rbuf.at[half], rbuf.at[half], pair_s.at[0], pair_r.at[0], pair)

    r_pair(core).start()

    def l_wait(k):
        l_copy(k, 2 * level(k) + yh).wait_recv()
        l_forward(k, 2 * level(k) + 1 - yh).wait_recv()

    each(1, Z, l_wait)
    fl[...] = lbuf[...].reshape(Q * 32, 128).astype(F32)
    for tile in range(4):
        parts = [fl[pl.ds(tile * 8 + r, Q, stride=32), :] for r in range(8)]
        block = jnp.concatenate(parts, axis=0)
        lt[:, tile * 128 : (tile + 1) * 128] = block.astype(BF)
        l2[tile * 128 : (tile + 1) * 128, :] = (block.T * (1.0 / S)).astype(BF)

    r_pair(1 - core).wait_recv()
    fr[...] = rbuf[...].reshape(2 * Q * 32, 128).astype(F32)
    low = lax.broadcasted_iota(jnp.int32, (S, 128), 1) < 64

    def make_blocks(t):
        parts = [
            fr[pl.ds(half * 512 + 2 * t + s, Q, stride=32), :] for half in range(2) for s in range(2)
        ]
        v = jnp.concatenate(parts, axis=0)
        u = pltpu.roll(v, 64, 1)
        zero = jnp.zeros_like(v)
        bd[t, :S, :128] = jnp.where(low, v, zero).astype(BF)
        bd[t, :S, 128:] = jnp.where(low, u, zero).astype(BF)
        bd[t, S:, :128] = jnp.where(low, zero, u).astype(BF)
        bd[t, S:, 128:] = jnp.where(low, zero, v).astype(BF)

    def outer(t):
        x = dot(l2[...], bd[t]).astype(BF)
        xb[:, 2 * t] = x[:, :128].reshape(Q, C, 128)
        xb[:, 2 * t + 1] = x[:, 128:].reshape(Q, C, 128)

    def some(count, step):
        def body(n):
            for m in range(count):
                step(n * count + m)

        return body

    each(0, 4, some(4, make_blocks))
    each(0, 4, some(4, outer))

    def grad_w(n):
        total = None
        for p in range(8):
            a = xb[2 * p, pl.ds(n * 8, 8)].reshape(256, 128)
            b = xb[2 * p + 1, pl.ds(n * 8, 8)].reshape(256, 128)
            term = dot(jnp.concatenate([a, b], axis=1), g[p * 256 : (p + 1) * 256, :])
            total = term if total is None else total + term
        gws[pl.ds(n * 8, 8)] = total.reshape(8, C, 128)

    each(0, 4, grad_w)

    def w_pair(half):
        src = gws.at[:, pl.ds(pl.multiple_of(half * Q, Q), Q), :]
        return remote(src, gwp, pair_s.at[1], pair_r.at[1], pair)

    w_pair(1 - core).start()

    def grad_r(t):
        y = jnp.concatenate([yb[:, 2 * t].reshape(512, 128), yb[:, 2 * t + 1].reshape(512, 128)], axis=1)
        x = dot(lt[...], y)
        a, b = x[:S, :128], x[S:, :128]
        c, d = x[:S, 128:], x[S:, 128:]
        grs[t] = jnp.where(low, a, d) + pltpu.roll(jnp.where(low, c, b), 64, 1)

    each(0, 4, some(4, grad_r))

    def g_pair(half):
        src = grs.at[:, pl.ds(pl.multiple_of(half * 32, 32), 32), :]
        return remote(src, grp, pair_s.at[2], pair_r.at[2], pair)

    g_pair(1 - core).start()

    def row_sends(sums, send_buf, recv_buf, send_sem, recv_sem):
        def fill(k):
            slot = chip(k)
            send_buf[slot] = sums[pl.ds(slot, 32, stride=Q), :].astype(BF)

        each(1, Q, fill)
        each(
            1, Q,
            lambda k: remote(
                send_buf.at[chip(k)], recv_buf.at[q], send_sem.at[k], recv_sem.at[q], row_mate(k)
            ).start(),
        )

    def row_wait(send_buf, recv_buf, send_sem, recv_sem):
        def one(k):
            remote(
                send_buf.at[chip(k)], recv_buf.at[chip(k)], send_sem.at[k], recv_sem.at[chip(k)], row_mate(k)
            ).wait_recv()

        each(1, Q, one)

    def row_total(sums, recv_buf):
        def add(k, acc):
            return acc + recv_buf[chip(k)].astype(F32)

        return lax.fori_loop(1, Q, add, sums[pl.ds(q, 32, stride=Q), :])

    w_pair(core).wait_recv()
    gwh[...] = (gws[:, pl.ds(pl.multiple_of(core * Q, Q), Q), :] + gwp[...]).reshape(512, 128)
    row_sends(gwh, gwsend, gwrecv, ws, wr)

    for tile in range(4):
        gls[tile] = jnp.zeros((128, 128), F32)

    def grad_l(n):
        total = None
        for m in range(4):
            t = n * 4 + m
            y = jnp.concatenate(
                [yb[:, 2 * t].reshape(512, 128), yb[:, 2 * t + 1].reshape(512, 128)], axis=1
            )
            term = dot(bd[t], y, ((1,), (1,)))
            total = term if total is None else total + term
        for tile in range(4):
            gls[tile] += total[:, tile * 128 : (tile + 1) * 128]

    each(0, 4, grad_l)

    g_pair(core).wait_recv()
    grh[...] = (grs[:, pl.ds(pl.multiple_of(core * 32, 32), 32), :] + grp[...]).reshape(512, 128)
    row_sends(grh, grsend, grrecv, gs, gr)

    def l_rows(c):
        return jnp.concatenate([gls[tile, pl.ds(c, 8, stride=Q), :] for tile in range(4)], axis=0)

    def fill_l(k):
        for side in range(2):
            glsend[level(k), side] = l_rows(2 * level(k) + side).astype(BF)

    each(1, Z, fill_l)

    def l_reduce(k, slot):
        return remote(glsend.at[level(k)], glrecv.at[slot], zls.at[k], zlr.at[slot], z_mate(k))

    each(1, Z, lambda k: l_reduce(k, z).start())

    row_wait(gwsend, gwrecv, ws, wr)
    total_w = row_total(gwh, gwrecv).astype(BF)
    gwzs[...] = total_w
    gwz[z] = total_w

    def w_level(k, slot):
        return remote(gwzs, gwz.at[slot], zws.at[k], zwr.at[slot], z_mate(k))

    each(1, Z, lambda k: w_level(k, z).start())

    each(1, Z, lambda k: l_reduce(k, level(k)).wait_recv())

    def l_total(side):
        def add(k, acc):
            return acc + glrecv[level(k), side].astype(F32)

        return lax.fori_loop(1, Z, add, l_rows(2 * z + side))

    glys[...] = l_total(1 - yh)
    side_l = remote(glys, gly, ys.at[0], yr.at[0], other)
    side_l.start()
    mine_l = l_total(yh)

    row_wait(grsend, grrecv, gs, gr)
    gr_out[...] = row_total(grh, grrecv) * (1.0 / S)

    each(1, Z, lambda k: w_level(k, level(k)).wait_recv())
    acc = gwz[0].astype(F32)
    for n in range(1, Z):
        acc = acc + gwz[n].astype(F32)
    gwys[...] = acc
    side_w = remote(gwys, gwy, ys.at[1], yr.at[1], other)
    side_w.start()

    side_l.wait_recv()
    gl_out[...] = (mine_l + gly[...]) * (1.0 / S)
    side_w.wait_recv()
    gw_out[...] = acc + gwy[...]

    l_side(col).wait_send()

    def finish_row(k):
        r_copy(k, q).wait_send()
        remote(gwsend.at[chip(k)], gwrecv.at[q], ws.at[k], wr.at[q], row_mate(k)).wait_send()
        remote(grsend.at[chip(k)], grrecv.at[q], gs.at[k], gr.at[q], row_mate(k)).wait_send()

    def finish_z(k):
        l_copy(k, col).wait_send()
        l_forward(k, side_col).wait_send()
        l_reduce(k, z).wait_send()
        w_level(k, z).wait_send()

    each(1, Q, finish_row)
    each(1, Z, finish_z)
    r_pair(core).wait_send()
    w_pair(1 - core).wait_send()
    g_pair(1 - core).wait_send()
    side_l.wait_send()
    side_w.wait_send()


def body(left_act, right_act, cotangent, weight):
    rmsg = right_act.reshape(16, 2, 2, 64).transpose(0, 2, 1, 3).reshape(32, 128)
    lmsg = left_act.reshape(16, 2, 4, 4, 4, 2).transpose(3, 5, 2, 4, 1, 0).reshape(32, 128)
    vm = pltpu.VMEM
    dma = pltpu.SemaphoreType.DMA
    msg = (32, 128)
    gl, gr, gw = pl.pallas_call(
        kernel,
        out_shape=[jax.ShapeDtypeStruct(msg, F32)] * 3,
        in_specs=[pl.BlockSpec(memory_space=vm)] * 4,
        out_specs=[pl.BlockSpec(memory_space=vm)] * 3,
        scratch_shapes=[
            vm((2, Q, *msg), BF), vm((16, *msg), BF),
            vm((1024, 128), F32), vm((512, 128), F32), vm((1024, 128), F32), vm((1024, 128), BF),
            vm((128, 512), BF), vm((512, 128), BF), vm((16, 128, 256), BF),
            vm((16, C, C, 128), BF), vm((16, C, C, 128), BF),
            vm((C, C, 128), F32), vm((C, Q, 128), F32), vm((512, 128), F32),
            vm((Q, *msg), BF), vm((Q, *msg), BF), vm((Z, *msg), BF), vm(msg, BF), vm(msg, F32), vm(msg, F32),
            vm((16, S, 128), F32), vm((16, 32, 128), F32), vm((512, 128), F32),
            vm((Q, *msg), BF), vm((Q, *msg), BF),
            vm((4, 128, 128), F32), vm((Z, 2, *msg), BF), vm((Z, 2, *msg), BF), vm(msg, F32), vm(msg, F32),
            dma((Q,)), dma((Q,)), dma((Z,)), dma((Z,)), dma((16,)), dma((3,)), dma((3,)),
            dma((Q,)), dma((Q,)), dma((Q,)), dma((Q,)),
            dma((Z,)), dma((Z,)), dma((Z,)), dma((Z,)), dma((2,)), dma((2,)),
        ],
        compiler_params=pltpu.CompilerParams(collective_id=0, has_side_effects=True),
    )(rmsg, lmsg, cotangent.reshape(2048, 128), weight)
    grad_left = gl.reshape(4, 2, 4, 4, 2, 16).transpose(5, 4, 2, 0, 3, 1).reshape(32, 4, 32)
    grad_right = gr.reshape(16, 2, 2, 64).transpose(0, 2, 1, 3).reshape(32, 2, 64)
    return grad_left, grad_right, gw


def solution(mesh):
    return jax.shard_map(
        body,
        mesh=mesh,
        in_specs=(P(None, "col", "row"), P(None, "row", "col"), P("row", "col", None), P()),
        out_specs=(P(None, "col", "row"), P(None, "row", "col"), P("row", None)),
        check_vma=False,
    )
```

```python
import jax
import jax.numpy as jnp
from jax import lax
from jax.experimental import pallas as pl
from jax.experimental.pallas import tpu as pltpu
from jax.sharding import PartitionSpec as P

BF = jnp.bfloat16
F32 = jnp.float32
MESH = pl.DeviceIdType.MESH
S = 64
C = 32
Q = 16
Z = 8
R_ROW, R_PAIR, L_SIDE, L_LEVEL, W_PAIR, W_ROW, W_LEVEL, G_PAIR, G_ROW, L_SUM, L_SUM_SIDE, W_SIDE = range(12)


def dot(a, b, dims=((1,), (0,))):
    return lax.dot_general(a, b, (dims, ((), ())), preferred_element_type=F32)


def swap_groups(parts, group):
    outs = []
    for s in range(4):
        out = None
        for a in range(4):
            shift = (a - s) % 4 * 32
            moved = pltpu.roll(parts[a], shift, 1) if shift else parts[a]
            out = moved if out is None else jnp.where(group == a, moved, out)
        outs.append(out)
    return outs


def kernel(
    l_in, r_in, g_in, w_in,
    gl_out, gr_out, gw_out,
    lv, rv, g, w, ra, la, lb, rmsg, lmsg,
    rbuf, lbuf, fr, fl, wf, wp, lt, l2, bd, xb, yb,
    gws, gwp, gwh, gwsend, gwrecv, gwz, gwzs, gwy, gwys,
    grs, grp, grh, grsend, grrecv, grf,
    gls, glsend, glrecv, gly, glys, glf, gt, ga,
    gwo, gro, glo, in_sem, out_sem, sent, got,
):
    row, col = lax.axis_index("row"), lax.axis_index("col")
    core, q = lax.rem(row, 2), row // 2
    yh, z = lax.rem(col, 2), col // 2
    pair = (row + 1 - 2 * core, col)
    other = (row, col + 1 - 2 * yh)

    def chip(k):
        return lax.rem(q + k, Q)

    def level(k):
        return lax.rem(z + k, Z)

    def row_mate(k):
        return (2 * chip(k) + core, col)

    def z_mate(k):
        return (row, 2 * level(k) + yh)

    def remote(src, dst, n, device):
        return pltpu.make_async_remote_copy(
            src_ref=src, dst_ref=dst, send_sem=sent.at[n], recv_sem=got.at[n],
            device_id=device, device_id_type=MESH,
        )

    def batch(buf, count, n):
        part = buf.at[pl.ds(0, count)]
        return remote(part, part, n, pair)

    def each(first, last, step):
        def body(k, carry):
            step(k)
            return carry

        lax.fori_loop(first, last, body, 0)

    barrier = pltpu.get_barrier_semaphore()

    def greet(device):
        pl.semaphore_signal(barrier, inc=1, device_id=device, device_id_type=MESH)

    each(1, Q, lambda k: greet(row_mate(k)))
    greet(other)
    each(1, Z, lambda k: greet(z_mate(k)))
    greet(pair)

    copies = [
        pltpu.make_async_copy(src, dst, in_sem.at[n])
        for n, (src, dst) in enumerate([(r_in, rv), (l_in, lv), (w_in, w), (g_in, g)])
    ]
    for copy in copies:
        copy.start()

    lane = lax.broadcasted_iota(jnp.int32, (S, 128), 1)
    low = lane < 64
    group = lane[:8] // 32

    ra[...] = jnp.zeros_like(ra)
    la[...] = jnp.zeros_like(la)
    copies[0].wait()
    for d in range(C):
        ra[2 * d : 2 * d + 2, :64] = rv[d].astype(F32)
    for s in range(2):
        a = ra[pl.ds(s, 16, stride=4), :]
        b = ra[pl.ds(2 + s, 16, stride=4), :]
        rmsg[s * 16 : s * 16 + 16, :] = jnp.where(low[:16], a, pltpu.roll(b, 64, 1)).astype(BF)

    copies[1].wait()
    for c in range(C):
        la[4 * c : 4 * c + 4, :32] = lv[c].astype(F32)
    stack = [la[pl.ds(half * 4 + s, Q, stride=8), :] for s in range(4) for half in range(2)]
    lb[...] = jnp.concatenate(stack, axis=0).T[:32]
    parts = [
        jnp.concatenate([lb[pl.ds(2 * a + n, 4, stride=8), :] for n in range(2)], axis=0)
        for a in range(4)
    ]
    lmsg[...] = jnp.concatenate(swap_groups(parts, group), axis=0).astype(BF)
    rbuf[core, q] = rmsg[...]
    lbuf[col] = lmsg[...]

    pl.semaphore_wait(barrier, Q + Z)

    side_col = col + 1 - 2 * yh
    l_side = remote(lmsg, lbuf.at[col], L_SIDE, other)
    l_side.start()
    each(1, Z, lambda k: remote(lmsg, lbuf.at[col], L_LEVEL, z_mate(k)).start())
    r_slots = rbuf.at[core]
    each(1, Q, lambda k: remote(rmsg, r_slots.at[q], R_ROW, row_mate(k)).start())

    copies[2].wait()
    wf[...] = w[...].astype(F32)

    def order_weight(d):
        for half in range(2):
            rows = wf[pl.ds(half * C + d, Q, stride=2 * C), :]
            wp[pl.ds(pl.multiple_of(d * C + half * Q, Q), Q), :] = rows.astype(BF)

    def some(count, step):
        def body(n):
            for m in range(count):
                step(n * count + m)

        return body

    each(0, C // 8, some(8, order_weight))
    copies[3].wait()

    def grad_outer(p):
        gp = g[pl.ds(pl.multiple_of(p * 256, 256), 256), :]
        y = dot(wp[...], gp, ((1,), (1,))).astype(BF)
        yb[2 * p] = y[:, :128].reshape(C, C, 128)
        yb[2 * p + 1] = y[:, 128:].reshape(C, C, 128)

    each(0, 8, grad_outer)

    l_side.wait_recv()
    forward = lbuf.at[side_col]
    each(1, Z, lambda k: remote(forward, forward, L_LEVEL, z_mate(k)).start())

    batch(r_slots, Q - 1, R_ROW).wait_recv()
    r_pair = remote(r_slots, r_slots, R_PAIR, pair)
    r_pair.start()

    r_pair.wait_recv()
    fr[...] = rbuf[...].reshape(2 * Q * 32, 128).astype(F32)

    def make_blocks(t):
        rows = [
            fr[pl.ds(half * 512 + s * 16 + t, Q, stride=32), :] for half in range(2) for s in range(2)
        ]
        v = jnp.concatenate(rows, axis=0)
        u = pltpu.roll(v, 64, 1)
        zero = jnp.zeros_like(v)
        bd[t, :S, :128] = jnp.where(low, v, zero).astype(BF)
        bd[t, :S, 128:] = jnp.where(low, u, zero).astype(BF)
        bd[t, S:, :128] = jnp.where(low, zero, u).astype(BF)
        bd[t, S:, 128:] = jnp.where(low, zero, v).astype(BF)

    each(0, 4, some(4, make_blocks))

    batch(lbuf, 2 * (Z - 1), L_LEVEL).wait_recv()
    fl[...] = lbuf[...].reshape(Q * 32, 128).astype(F32)
    for tile in range(4):
        rows = [
            fl[pl.ds(s * 8 + n * 4 + tile, Q, stride=32), :] for n in range(2) for s in range(4)
        ]
        block = jnp.concatenate(rows, axis=0)
        lt[:, tile * 128 : (tile + 1) * 128] = block.astype(BF)
        l2[tile * 128 : (tile + 1) * 128, :] = (block.T * (1.0 / S)).astype(BF)

    def outer(t):
        x = dot(l2[...], bd[t]).astype(BF)
        xb[:, 2 * t] = x[:, :128].reshape(Q, C, 128)
        xb[:, 2 * t + 1] = x[:, 128:].reshape(Q, C, 128)

    def grad_w(n):
        total = None
        for p in range(8):
            a = xb[2 * p, pl.ds(n * 8, 8)].reshape(256, 128)
            b = xb[2 * p + 1, pl.ds(n * 8, 8)].reshape(256, 128)
            term = dot(jnp.concatenate([a, b], axis=1), g[p * 256 : (p + 1) * 256, :])
            total = term if total is None else total + term
        gws[pl.ds(n * 8, 8)] = total.reshape(8, C, 128)

    for t in range(16):
        outer(t)
    for n in range(4):
        grad_w(n)
    w_pair = remote(gws.at[:, pl.ds(pl.multiple_of((1 - core) * Q, Q), Q), :], gwp, W_PAIR, pair)
    w_pair.start()

    def grad_r(t):
        y = jnp.concatenate([yb[:, 2 * t].reshape(512, 128), yb[:, 2 * t + 1].reshape(512, 128)], axis=1)
        x = dot(lt[...], y)
        a, b = x[:S, :128], x[S:, :128]
        c, d = x[:S, 128:], x[S:, 128:]
        grs[t] = jnp.where(low, a, d) + pltpu.roll(jnp.where(low, c, b), 64, 1)

    each(0, 2, some(4, grad_r))
    w_pair.wait_recv()
    gwh[...] = (gws[:, pl.ds(pl.multiple_of(core * Q, Q), Q), :] + gwp[...]).reshape(512, 128)

    def fill_w(k):
        gwsend[k] = gwh[pl.ds(k, 32, stride=Q), :].astype(BF)

    each(0, 2, some(8, fill_w))
    each(1, Q, lambda k: remote(gwsend.at[chip(k)], gwrecv.at[q], W_ROW, row_mate(k)).start())
    each(2, 4, some(4, grad_r))

    g_pair = remote(grs.at[:, pl.ds(pl.multiple_of((1 - core) * 32, 32), 32), :], grp, G_PAIR, pair)
    g_pair.start()

    for tile in range(4):
        gls[tile] = jnp.zeros((128, 128), F32)

    def grad_l(n):
        total = None
        for m in range(4):
            t = n * 4 + m
            y = jnp.concatenate(
                [yb[:, 2 * t].reshape(512, 128), yb[:, 2 * t + 1].reshape(512, 128)], axis=1
            )
            term = dot(bd[t], y, ((1,), (1,)))
            total = term if total is None else total + term
        for tile in range(4):
            gls[tile] += total[:, tile * 128 : (tile + 1) * 128]

    each(0, 4, grad_l)

    g_pair.wait_recv()
    grh[...] = (grs[:, pl.ds(pl.multiple_of(core * 32, 32), 32), :] + grp[...]).reshape(512, 128)

    def fill_g(k):
        grsend[chip(k)] = grh[pl.ds(chip(k), 32, stride=Q), :].astype(BF)

    each(0, 4, some(4, fill_g))
    each(1, Q, lambda k: remote(grsend.at[chip(k)], grrecv.at[q], G_ROW, row_mate(k)).start())

    def l_rows(c):
        return jnp.concatenate([gls[tile, pl.ds(c, 8, stride=Q), :] for tile in range(4)], axis=0)

    def fill_l(k):
        for side in range(2):
            glsend[level(k), side] = l_rows(2 * level(k) + side).astype(BF)

    each(0, 2, some(4, fill_l))

    each(1, Z, lambda k: remote(glsend.at[level(k)], glrecv.at[z], L_SUM, z_mate(k)).start())

    batch(gwrecv, Q - 1, W_ROW).wait_recv()
    acc = gwh[pl.ds(q, 32, stride=Q), :]
    for k in range(1, Q):
        acc = acc + gwrecv[chip(k)].astype(F32)
    total_w = acc.astype(BF)
    gwzs[...] = total_w
    gwz[z] = total_w
    each(1, Z, lambda k: remote(gwzs, gwz.at[z], W_LEVEL, z_mate(k)).start())

    batch(glrecv, Z - 1, L_SUM).wait_recv()

    def l_total(side):
        acc = l_rows(2 * z + side)
        for k in range(1, Z):
            acc = acc + glrecv[level(k), side].astype(F32)
        return acc

    glys[...] = l_total(1 - yh)
    side_l = remote(glys, gly, L_SUM_SIDE, other)
    side_l.start()
    glf[...] = l_total(yh)

    batch(grrecv, Q - 1, G_ROW).wait_recv()
    acc_r = grh[pl.ds(q, 32, stride=Q), :]
    for k in range(1, Q):
        acc_r = acc_r + grrecv[chip(k)].astype(F32)
    acc_r = acc_r * (1.0 / S)
    grf[0] = acc_r
    grf[1] = pltpu.roll(acc_r, 64, 1)
    for t in range(16):
        for dd in range(2):
            gro[2 * t + dd] = grf[dd, 2 * t : 2 * t + 2, :64]
    put_r = pltpu.make_async_copy(gro, gr_out, out_sem.at[0])
    put_r.start()

    gt[...] = jnp.zeros_like(gt)
    batch(gwz, Z - 1, W_LEVEL).wait_recv()
    acc = gwz[0].astype(F32)
    for n in range(1, Z):
        acc = acc + gwz[n].astype(F32)
    gwys[...] = acc
    side_w = remote(gwys, gwy, W_SIDE, other)
    side_w.start()
    side_l.wait_recv()
    glf[...] = (glf[...] + gly[...]) * (1.0 / S)
    parts = swap_groups([glf[pl.ds(s, 8, stride=4), :] for s in range(4)], group)
    for a in range(4):
        for tile in range(4):
            gt[tile * 8 + 2 * a : tile * 8 + 2 * a + 2, :] = parts[a][2 * tile : 2 * tile + 2]
    ga[...] = gt[...].T
    for c in range(C):
        glo[c] = ga[pl.ds(c % 2 * Q + c // 2, 4, stride=32), :][:, :32]
    put_l = pltpu.make_async_copy(glo, gl_out, out_sem.at[1])
    put_l.start()

    side_w.wait_recv()
    gwo[...] = gwys[...] + gwy[...]
    put_w = pltpu.make_async_copy(gwo, gw_out, out_sem.at[2])
    put_w.start()

    batch(r_slots, Q - 1, R_ROW).wait_send()
    l_side.wait_send()
    batch(lbuf, 2 * (Z - 1), L_LEVEL).wait_send()
    r_pair.wait_send()
    w_pair.wait_send()
    batch(gwrecv, Q - 1, W_ROW).wait_send()
    side_w.wait_send()
    g_pair.wait_send()
    batch(grsend, Q - 1, G_ROW).wait_send()
    batch(glsend, Z - 1, L_SUM).wait_send()
    side_l.wait_send()
    batch(gwz, Z - 1, W_LEVEL).wait_send()
    put_r.wait()
    put_l.wait()
    put_w.wait()


def body(left_act, right_act, cotangent, weight):
    vm = pltpu.VMEM
    dma = pltpu.SemaphoreType.DMA
    msg = (32, 128)
    return pl.pallas_call(
        kernel,
        out_shape=[
            jax.ShapeDtypeStruct(left_act.shape, F32),
            jax.ShapeDtypeStruct(right_act.shape, F32),
            jax.ShapeDtypeStruct(msg, F32),
        ],
        in_specs=[pl.BlockSpec(memory_space=pltpu.HBM)] * 4,
        out_specs=[pl.BlockSpec(memory_space=pltpu.HBM)] * 3,
        scratch_shapes=[
            vm((C, 4, 32), BF), vm((C, 2, 64), BF), vm((2048, 128), BF), vm((1024, 128), BF),
            vm((64, 128), F32), vm((128, 128), F32), vm(msg, F32), vm(msg, BF), vm(msg, BF),
            vm((2, Q, *msg), BF), vm((16, *msg), BF),
            vm((1024, 128), F32), vm((512, 128), F32), vm((1024, 128), F32), vm((1024, 128), BF),
            vm((128, 512), BF), vm((512, 128), BF), vm((16, 128, 256), BF),
            vm((16, C, C, 128), BF), vm((16, C, C, 128), BF),
            vm((C, C, 128), F32), vm((C, Q, 128), F32), vm((512, 128), F32),
            vm((Q, *msg), BF), vm((Q, *msg), BF), vm((Z, *msg), BF), vm(msg, BF), vm(msg, F32), vm(msg, F32),
            vm((16, S, 128), F32), vm((16, 32, 128), F32), vm((512, 128), F32),
            vm((Q, *msg), BF), vm((Q, *msg), BF), vm((2, *msg), F32),
            vm((4, 128, 128), F32), vm((Z, 2, *msg), BF), vm((Z, 2, *msg), BF), vm(msg, F32), vm(msg, F32),
            vm(msg, F32), vm((128, 128), F32), vm((128, 128), F32),
            vm(msg, F32), vm((C, 2, 64), F32), vm((C, 4, 32), F32), dma((4,)), dma((3,)), dma((12,)), dma((12,)),
        ],
        compiler_params=pltpu.CompilerParams(
            collective_id=0, has_side_effects=True
        ),
    )(left_act, right_act, cotangent.reshape(2048, 128), weight)


def solution(mesh):
    return jax.shard_map(
        body,
        mesh=mesh,
        in_specs=(P(None, "col", "row"), P(None, "row", "col"), P("row", "col", None), P()),
        out_specs=(P(None, "col", "row"), P(None, "row", "col"), P("row", None)),
        check_vma=False,
    )
```

```python
import jax
import jax.numpy as jnp
from jax import lax
from jax.experimental import pallas as pl
from jax.experimental.pallas import tpu as pltpu
from jax.sharding import PartitionSpec as P

BF = jnp.bfloat16
F32 = jnp.float32
MESH = pl.DeviceIdType.MESH
S = 64
C = 32
Q = 16
Z = 8
R_ROW, R_PAIR, L_SIDE, L_LEVEL, W_X, W_Y, W_LEVEL, G_PAIR, G_ROW, L_SUM, L_SUM_SIDE = range(11)


def dot(a, b, dims=((1,), (0,))):
    return lax.dot_general(a, b, (dims, ((), ())), preferred_element_type=F32)


def swap_groups(parts, group):
    outs = []
    for s in range(4):
        out = None
        for a in range(4):
            shift = (a - s) % 4 * 32
            moved = pltpu.roll(parts[a], shift, 1) if shift else parts[a]
            out = moved if out is None else jnp.where(group == a, moved, out)
        outs.append(out)
    return outs


def kernel(
    l_in, r_in, g_in, w_in,
    gl_out, gr_out, gw_out,
    lv, rv, g, w, ra, la, lb, rmsg, lmsg,
    rbuf, lbuf, fr, fl, wf, wp, lt, l2, bd, xb, yb,
    gws, gwsend, gwx, gwysend, gwy, gwz, gwzs,
    grs, grp, grh, grsend, grrecv, grf,
    gls, glsend, glrecv, gly, glys, glf, gt, ga,
    gwo, gro, glo, in_sem, out_sem, sent, got,
):
    row, col = lax.axis_index("row"), lax.axis_index("col")
    core, q = lax.rem(row, 2), row // 2
    yh, z = lax.rem(col, 2), col // 2
    me_x, me_y = lax.rem(row, 8), 4 * yh + row // 8
    pair = (row + 1 - 2 * core, col)
    other = (row, col + 1 - 2 * yh)

    def chip(k):
        return lax.rem(q + k, Q)

    def level(k):
        return lax.rem(z + k, Z)

    def row_mate(k):
        return (2 * chip(k) + core, col)

    def z_mate(k):
        return (row, 2 * level(k) + yh)

    def remote(src, dst, n, device):
        return pltpu.make_async_remote_copy(
            src_ref=src, dst_ref=dst, send_sem=sent.at[n], recv_sem=got.at[n],
            device_id=device, device_id_type=MESH,
        )

    def batch(buf, count, n):
        part = buf.at[pl.ds(0, count)]
        return remote(part, part, n, pair)

    def each(first, last, step):
        def body(k, carry):
            step(k)
            return carry

        lax.fori_loop(first, last, body, 0)

    barrier = pltpu.get_barrier_semaphore()

    def greet(device):
        pl.semaphore_signal(barrier, inc=1, device_id=device, device_id_type=MESH)

    each(1, Q, lambda k: greet(row_mate(k)))
    greet(other)
    each(1, Z, lambda k: greet(z_mate(k)))
    greet(pair)

    copies = [
        pltpu.make_async_copy(src, dst, in_sem.at[n])
        for n, (src, dst) in enumerate([(r_in, rv), (l_in, lv), (w_in, w), (g_in, g)])
    ]
    for copy in copies:
        copy.start()

    lane = lax.broadcasted_iota(jnp.int32, (S, 128), 1)
    low = lane < 64
    group = lane[:8] // 32

    ra[...] = jnp.zeros_like(ra)
    la[...] = jnp.zeros_like(la)
    copies[0].wait()
    for d in range(C):
        ra[2 * d : 2 * d + 2, :64] = rv[d].astype(F32)
    for s in range(2):
        a = ra[pl.ds(s, 16, stride=4), :]
        b = ra[pl.ds(2 + s, 16, stride=4), :]
        rmsg[s * 16 : s * 16 + 16, :] = jnp.where(low[:16], a, pltpu.roll(b, 64, 1)).astype(BF)

    copies[1].wait()
    for c in range(C):
        la[4 * c : 4 * c + 4, :32] = lv[c].astype(F32)
    stack = [la[pl.ds(half * 4 + s, Q, stride=8), :] for s in range(4) for half in range(2)]
    lb[...] = jnp.concatenate(stack, axis=0).T[:32]
    parts = [
        jnp.concatenate([lb[pl.ds(2 * a + n, 4, stride=8), :] for n in range(2)], axis=0)
        for a in range(4)
    ]
    lmsg[...] = jnp.concatenate(swap_groups(parts, group), axis=0).astype(BF)
    rbuf[core, q] = rmsg[...]
    lbuf[col] = lmsg[...]

    pl.semaphore_wait(barrier, Q + Z)

    side_col = col + 1 - 2 * yh
    l_side = remote(lmsg, lbuf.at[col], L_SIDE, other)
    l_side.start()
    each(1, Z, lambda k: remote(lmsg, lbuf.at[col], L_LEVEL, z_mate(k)).start())
    r_slots = rbuf.at[core]
    each(1, Q, lambda k: remote(rmsg, r_slots.at[q], R_ROW, row_mate(k)).start())

    copies[2].wait()
    wf[...] = w[...].astype(F32)

    def order_weight(d):
        for half in range(2):
            rows = wf[pl.ds(half * C + d, Q, stride=2 * C), :]
            wp[pl.ds(pl.multiple_of(d * C + half * Q, Q), Q), :] = rows.astype(BF)

    def some(count, step):
        def body(n):
            for m in range(count):
                step(n * count + m)

        return body

    each(0, C // 8, some(8, order_weight))
    copies[3].wait()

    def grad_outer(p):
        gp = g[pl.ds(pl.multiple_of(p * 256, 256), 256), :]
        y = dot(wp[...], gp, ((1,), (1,))).astype(BF)
        yb[2 * p] = y[:, :128].reshape(C, C, 128)
        yb[2 * p + 1] = y[:, 128:].reshape(C, C, 128)

    each(0, 8, grad_outer)

    l_side.wait_recv()
    forward = lbuf.at[side_col]
    each(1, Z, lambda k: remote(forward, forward, L_LEVEL, z_mate(k)).start())

    batch(r_slots, Q - 1, R_ROW).wait_recv()
    r_pair = remote(r_slots, r_slots, R_PAIR, pair)
    r_pair.start()

    r_pair.wait_recv()
    fr[...] = rbuf[...].reshape(2 * Q * 32, 128).astype(F32)

    def make_blocks(t):
        rows = [
            fr[pl.ds(half * 512 + s * 16 + t, Q, stride=32), :] for half in range(2) for s in range(2)
        ]
        v = jnp.concatenate(rows, axis=0)
        u = pltpu.roll(v, 64, 1)
        zero = jnp.zeros_like(v)
        bd[t, :S, :128] = jnp.where(low, v, zero).astype(BF)
        bd[t, :S, 128:] = jnp.where(low, u, zero).astype(BF)
        bd[t, S:, :128] = jnp.where(low, zero, u).astype(BF)
        bd[t, S:, 128:] = jnp.where(low, zero, v).astype(BF)

    each(0, 4, some(4, make_blocks))

    batch(lbuf, 2 * (Z - 1), L_LEVEL).wait_recv()
    fl[...] = lbuf[...].reshape(Q * 32, 128).astype(F32)
    for tile in range(4):
        rows = [
            fl[pl.ds(s * 8 + n * 4 + tile, Q, stride=32), :] for n in range(2) for s in range(4)
        ]
        block = jnp.concatenate(rows, axis=0)
        lt[:, tile * 128 : (tile + 1) * 128] = block.astype(BF)
        l2[tile * 128 : (tile + 1) * 128, :] = (block.T * (1.0 / S)).astype(BF)

    def outer(t):
        x = dot(l2[...], bd[t]).astype(BF)
        xb[:, 2 * t] = x[:, :128].reshape(Q, C, 128)
        xb[:, 2 * t + 1] = x[:, 128:].reshape(Q, C, 128)

    def grad_w(n):
        total = None
        for p in range(8):
            a = xb[2 * p, pl.ds(n * 8, 8)].reshape(256, 128)
            b = xb[2 * p + 1, pl.ds(n * 8, 8)].reshape(256, 128)
            term = dot(jnp.concatenate([a, b], axis=1), g[p * 256 : (p + 1) * 256, :])
            total = term if total is None else total + term
        gws[pl.ds(pl.multiple_of(n * 256, 256), 256), :] = total

    for t in range(16):
        outer(t)
    for n in range(4):
        grad_w(n)
    def fill_w(m):
        for n in range(4):
            gwsend[m, n] = gws[pl.ds(lax.rem(m, 2) * Q + n * 4 + m // 2, 32, stride=C), :].astype(BF)

    def x_mate(k):
        return lax.rem(me_x + k, 8)

    each(0, 4, some(2, fill_w))
    each(
        1, 8,
        lambda k: remote(gwsend.at[x_mate(k)], gwx.at[me_x], W_X, (row - me_x + x_mate(k), col)).start(),
    )

    def grad_r(t):
        y = jnp.concatenate([yb[:, 2 * t].reshape(512, 128), yb[:, 2 * t + 1].reshape(512, 128)], axis=1)
        x = dot(lt[...], y)
        a, b = x[:S, :128], x[S:, :128]
        c, d = x[:S, 128:], x[S:, 128:]
        grs[t] = jnp.where(low, a, d) + pltpu.roll(jnp.where(low, c, b), 64, 1)

    each(0, 4, some(4, grad_r))

    g_pair = remote(grs.at[:, pl.ds(pl.multiple_of((1 - core) * 32, 32), 32), :], grp, G_PAIR, pair)
    g_pair.start()

    for tile in range(4):
        gls[tile] = jnp.zeros((128, 128), F32)

    def grad_l(n):
        total = None
        for m in range(4):
            t = n * 4 + m
            y = jnp.concatenate(
                [yb[:, 2 * t].reshape(512, 128), yb[:, 2 * t + 1].reshape(512, 128)], axis=1
            )
            term = dot(bd[t], y, ((1,), (1,)))
            total = term if total is None else total + term
        for tile in range(4):
            gls[tile] += total[:, tile * 128 : (tile + 1) * 128]

    each(0, 4, grad_l)

    g_pair.wait_recv()
    grh[...] = (grs[:, pl.ds(pl.multiple_of(core * 32, 32), 32), :] + grp[...]).reshape(512, 128)

    def fill_g(k):
        grsend[chip(k)] = grh[pl.ds(chip(k), 32, stride=Q), :].astype(BF)

    each(0, 4, some(4, fill_g))

    def l_rows(c):
        return jnp.concatenate([gls[tile, pl.ds(c, 8, stride=Q), :] for tile in range(4)], axis=0)

    def fill_l(k):
        for side in range(2):
            glsend[level(k), side] = l_rows(2 * level(k) + side).astype(BF)

    each(0, 2, some(4, fill_l))

    each(1, Z, lambda k: remote(glsend.at[level(k)], glrecv.at[z], L_SUM, z_mate(k)).start())

    batch(gwx, 7, W_X).wait_recv()
    for n in range(4):
        acc = gws[pl.ds(core * Q + n * 4 + me_x // 2, 32, stride=C), :]
        for k in range(1, 8):
            acc = acc + gwx[x_mate(k), n].astype(F32)
        gwysend[n] = acc.astype(BF)

    def y_mate(k):
        there = lax.rem(me_y + k, 8)
        return lax.rem(there, 4), (lax.rem(there, 4) * 8 + me_x, 2 * z + there // 4)

    each(1, 8, lambda k: remote(gwysend.at[y_mate(k)[0]], gwy.at[me_y], W_Y, y_mate(k)[1]).start())
    each(1, Q, lambda k: remote(grsend.at[chip(k)], grrecv.at[q], G_ROW, row_mate(k)).start())
    gwy[me_y] = gwysend[lax.rem(me_y, 4)]
    batch(gwy, 7, W_Y).wait_recv()
    acc = gwy[0].astype(F32)
    for n in range(1, 8):
        acc = acc + gwy[n].astype(F32)
    gwzs[...] = acc
    gwz[z] = acc
    each(1, Z, lambda k: remote(gwzs, gwz.at[z], W_LEVEL, z_mate(k)).start())

    batch(glrecv, Z - 1, L_SUM).wait_recv()

    def l_total(side):
        acc = l_rows(2 * z + side)
        for k in range(1, Z):
            acc = acc + glrecv[level(k), side].astype(F32)
        return acc

    glys[...] = l_total(1 - yh)
    side_l = remote(glys, gly, L_SUM_SIDE, other)
    side_l.start()
    glf[...] = l_total(yh)

    batch(grrecv, Q - 1, G_ROW).wait_recv()
    acc_r = grh[pl.ds(q, 32, stride=Q), :]
    for k in range(1, Q):
        acc_r = acc_r + grrecv[chip(k)].astype(F32)
    acc_r = acc_r * (1.0 / S)
    grf[0] = acc_r
    grf[1] = pltpu.roll(acc_r, 64, 1)
    for t in range(16):
        for dd in range(2):
            gro[2 * t + dd] = grf[dd, 2 * t : 2 * t + 2, :64]
    put_r = pltpu.make_async_copy(gro, gr_out, out_sem.at[0])
    put_r.start()

    gt[...] = jnp.zeros_like(gt)
    side_l.wait_recv()
    glf[...] = (glf[...] + gly[...]) * (1.0 / S)
    parts = swap_groups([glf[pl.ds(s, 8, stride=4), :] for s in range(4)], group)
    for a in range(4):
        for tile in range(4):
            gt[tile * 8 + 2 * a : tile * 8 + 2 * a + 2, :] = parts[a][2 * tile : 2 * tile + 2]
    ga[...] = gt[...].T
    for c in range(C):
        glo[c] = ga[pl.ds(c % 2 * Q + c // 2, 4, stride=32), :][:, :32]
    put_l = pltpu.make_async_copy(glo, gl_out, out_sem.at[1])
    put_l.start()

    batch(gwz, Z - 1, W_LEVEL).wait_recv()
    acc = gwz[0]
    for n in range(1, Z):
        acc = acc + gwz[n]
    gwo[...] = acc
    put_w = pltpu.make_async_copy(gwo, gw_out, out_sem.at[2])
    put_w.start()

    batch(r_slots, Q - 1, R_ROW).wait_send()
    l_side.wait_send()
    batch(lbuf, 2 * (Z - 1), L_LEVEL).wait_send()
    r_pair.wait_send()
    batch(gwsend, 7, W_X).wait_send()
    batch(gwy, 7, W_Y).wait_send()
    g_pair.wait_send()
    batch(grsend, Q - 1, G_ROW).wait_send()
    batch(glsend, Z - 1, L_SUM).wait_send()
    side_l.wait_send()
    batch(gwz, Z - 1, W_LEVEL).wait_send()
    put_r.wait()
    put_l.wait()
    put_w.wait()


def put(a_in, b_in, c_in, a_out, b_out, c_out, a, b, c, in_sem, out_sem):
    sides = [(a_in, a, a_out), (b_in, b, b_out), (c_in, c, c_out)]
    reads = [pltpu.make_async_copy(src, mid, in_sem.at[n]) for n, (src, mid, _) in enumerate(sides)]
    writes = [pltpu.make_async_copy(mid, dst, out_sem.at[n]) for n, (_, mid, dst) in enumerate(sides)]
    for read in reads:
        read.start()
    for read, write in zip(reads, writes):
        read.wait()
        write.start()
    for write in writes:
        write.wait()


def body(left_act, right_act, cotangent, weight):
    vm = pltpu.VMEM
    dma = pltpu.SemaphoreType.DMA
    msg = (32, 128)
    parts = pl.pallas_call(
        kernel,
        out_shape=[
            jax.ShapeDtypeStruct(left_act.shape, F32),
            jax.ShapeDtypeStruct(right_act.shape, F32),
            jax.ShapeDtypeStruct(msg, F32),
        ],
        in_specs=[pl.BlockSpec(memory_space=pltpu.HBM)] * 4,
        out_specs=[pl.BlockSpec(memory_space=pltpu.HBM)] * 3,
        scratch_shapes=[
            vm((C, 4, 32), BF), vm((C, 2, 64), BF), vm((2048, 128), BF), vm((1024, 128), BF),
            vm((64, 128), F32), vm((128, 128), F32), vm(msg, F32), vm(msg, BF), vm(msg, BF),
            vm((2, Q, *msg), BF), vm((16, *msg), BF),
            vm((1024, 128), F32), vm((512, 128), F32), vm((1024, 128), F32), vm((1024, 128), BF),
            vm((128, 512), BF), vm((512, 128), BF), vm((16, 128, 256), BF),
            vm((16, C, C, 128), BF), vm((16, C, C, 128), BF),
            vm((1024, 128), F32), vm((8, 4, *msg), BF), vm((8, 4, *msg), BF),
            vm((4, *msg), BF), vm((8, *msg), BF), vm((Z, *msg), F32), vm(msg, F32),
            vm((16, S, 128), F32), vm((16, 32, 128), F32), vm((512, 128), F32),
            vm((Q, *msg), BF), vm((Q, *msg), BF), vm((2, *msg), F32),
            vm((4, 128, 128), F32), vm((Z, 2, *msg), BF), vm((Z, 2, *msg), BF), vm(msg, F32), vm(msg, F32),
            vm(msg, F32), vm((128, 128), F32), vm((128, 128), F32),
            vm(msg, F32), vm((C, 2, 64), F32), vm((C, 4, 32), F32), dma((4,)), dma((3,)), dma((11,)), dma((11,)),
        ],
        compiler_params=pltpu.CompilerParams(
            collective_id=0, has_side_effects=True
        ),
    )(left_act, right_act, cotangent.reshape(2048, 128), weight)
    shapes = [part.shape for part in parts]
    return pl.pallas_call(
        put,
        out_shape=[jax.ShapeDtypeStruct(shape, F32) for shape in shapes],
        in_specs=[pl.BlockSpec(memory_space=pl.ANY)] * 3,
        out_specs=[pl.BlockSpec(memory_space=pl.ANY)] * 3,
        scratch_shapes=[*(vm(shape, F32) for shape in shapes), dma((3,)), dma((3,))],
    )(*parts)


def solution(mesh):
    return jax.shard_map(
        body,
        mesh=mesh,
        in_specs=(P(None, "col", "row"), P(None, "row", "col"), P("row", "col", None), P()),
        out_specs=(P(None, "col", "row"), P(None, "row", "col"), P("row", None)),
        check_vma=False,
    )
```

```python
import jax
import jax.numpy as jnp
from jax import lax
from jax.experimental import pallas as pl
from jax.experimental.pallas import tpu as pltpu
from jax.sharding import PartitionSpec as P

BF = jnp.bfloat16
F32 = jnp.float32
MESH = pl.DeviceIdType.MESH
S = 64
C = 32
Q = 16
Z = 8
FAR_FIRST = (4, 3, 5, 2, 6, 1, 7)
R_ROW, R_PAIR, L_SIDE, L_LEVEL, W_X, W_Y, W_LEVEL, G_PAIR, G_ROW, L_SUM, L_SUM_SIDE = range(11)


def dot(a, b, dims=((1,), (0,))):
    return lax.dot_general(a, b, (dims, ((), ())), preferred_element_type=F32)


def swap_groups(parts, group):
    outs = []
    for s in range(4):
        out = None
        for a in range(4):
            shift = (a - s) % 4 * 32
            moved = pltpu.roll(parts[a], shift, 1) if shift else parts[a]
            out = moved if out is None else jnp.where(group == a, moved, out)
        outs.append(out)
    return outs


def kernel(
    l_in, r_in, g_in, w_in,
    gl_out, gr_out, gw_out,
    lv, rv, g, w, ra, la, lb, rmsg, lmsg,
    rbuf, lbuf, fr, fl, wf, wp, lt, l2, bd, xb, yb,
    gws, gwsend, gwx, gwysend, gwy, gwz, gwzs,
    grs, grp, grh, grsend, grrecv, grf,
    gls, glsend, glrecv, gly, glys, glf, gt, ga,
    in_sem, sent, got,
):
    row, col = lax.axis_index("row"), lax.axis_index("col")
    core, q = lax.rem(row, 2), row // 2
    yh, z = lax.rem(col, 2), col // 2
    me_x, me_y = lax.rem(row, 8), 4 * yh + row // 8
    pair = (row + 1 - 2 * core, col)
    other = (row, col + 1 - 2 * yh)

    def chip(k):
        return lax.rem(q + k, Q)

    def level(k):
        return lax.rem(z + k, Z)

    def row_mate(k):
        return (2 * chip(k) + core, col)

    def z_mate(k):
        return (row, 2 * level(k) + yh)

    def remote(src, dst, n, device):
        return pltpu.make_async_remote_copy(
            src_ref=src, dst_ref=dst, send_sem=sent.at[n], recv_sem=got.at[n],
            device_id=device, device_id_type=MESH,
        )

    def batch(buf, count, n):
        part = buf.at[pl.ds(0, count)]
        return remote(part, part, n, pair)

    def each(first, last, step):
        def body(k, carry):
            step(k)
            return carry

        lax.fori_loop(first, last, body, 0)

    barrier = pltpu.get_barrier_semaphore()

    def greet(device):
        pl.semaphore_signal(barrier, inc=1, device_id=device, device_id_type=MESH)

    greet(other)
    for k in FAR_FIRST:
        greet(z_mate(k))
    each(1, Q, lambda k: greet(row_mate(k)))
    greet(pair)

    copies = [
        pltpu.make_async_copy(src, dst, in_sem.at[n])
        for n, (src, dst) in enumerate([(r_in, rv), (l_in, lv), (w_in, w), (g_in, g)])
    ]
    for copy in copies:
        copy.start()

    lane = lax.broadcasted_iota(jnp.int32, (S, 128), 1)
    low = lane < 64
    group = lane[:8] // 32

    ra[...] = jnp.zeros_like(ra)
    la[...] = jnp.zeros_like(la)
    copies[0].wait()
    for d in range(C):
        ra[2 * d : 2 * d + 2, :64] = rv[d].astype(F32)
    for s in range(2):
        a = ra[pl.ds(s, 16, stride=4), :]
        b = ra[pl.ds(2 + s, 16, stride=4), :]
        rmsg[s * 16 : s * 16 + 16, :] = jnp.where(low[:16], a, pltpu.roll(b, 64, 1)).astype(BF)

    copies[1].wait()
    for c in range(C):
        la[4 * c : 4 * c + 4, :32] = lv[c].astype(F32)
    stack = [la[pl.ds(half * 4 + s, Q, stride=8), :] for s in range(4) for half in range(2)]
    lb[...] = jnp.concatenate(stack, axis=0).T[:32]
    parts = [
        jnp.concatenate([lb[pl.ds(2 * a + n, 4, stride=8), :] for n in range(2)], axis=0)
        for a in range(4)
    ]
    lmsg[...] = jnp.concatenate(swap_groups(parts, group), axis=0).astype(BF)
    rbuf[core, q] = rmsg[...]
    lbuf[col] = lmsg[...]

    pl.semaphore_wait(barrier, Q + Z)

    side_col = col + 1 - 2 * yh
    l_side = remote(lmsg, lbuf.at[col], L_SIDE, other)
    l_side.start()
    for k in FAR_FIRST:
        remote(lmsg, lbuf.at[col], L_LEVEL, z_mate(k)).start()
    r_slots = rbuf.at[core]
    each(1, Q, lambda k: remote(rmsg, r_slots.at[q], R_ROW, row_mate(k)).start())

    copies[2].wait()
    wf[...] = w[...].astype(F32)

    def order_weight(d):
        for half in range(2):
            rows = wf[pl.ds(half * C + d, Q, stride=2 * C), :]
            wp[pl.ds(pl.multiple_of(d * C + half * Q, Q), Q), :] = rows.astype(BF)

    def some(count, step):
        def body(n):
            for m in range(count):
                step(n * count + m)

        return body

    each(0, C // 8, some(8, order_weight))
    copies[3].wait()

    def grad_outer(p):
        gp = g[pl.ds(pl.multiple_of(p * 256, 256), 256), :]
        y = dot(wp[...], gp, ((1,), (1,))).astype(BF)
        yb[2 * p] = y[:, :128].reshape(C, C, 128)
        yb[2 * p + 1] = y[:, 128:].reshape(C, C, 128)

    each(0, 8, grad_outer)

    l_side.wait_recv()
    forward = lbuf.at[side_col]
    for k in FAR_FIRST:
        remote(forward, forward, L_LEVEL, z_mate(k)).start()

    batch(r_slots, Q - 1, R_ROW).wait_recv()
    r_pair = remote(r_slots, r_slots, R_PAIR, pair)
    r_pair.start()

    r_pair.wait_recv()
    fr[...] = rbuf[...].reshape(2 * Q * 32, 128).astype(F32)

    def make_blocks(t):
        rows = [
            fr[pl.ds(half * 512 + s * 16 + t, Q, stride=32), :] for half in range(2) for s in range(2)
        ]
        v = jnp.concatenate(rows, axis=0)
        u = pltpu.roll(v, 64, 1)
        zero = jnp.zeros_like(v)
        bd[t, :S, :128] = jnp.where(low, v, zero).astype(BF)
        bd[t, :S, 128:] = jnp.where(low, u, zero).astype(BF)
        bd[t, S:, :128] = jnp.where(low, zero, u).astype(BF)
        bd[t, S:, 128:] = jnp.where(low, zero, v).astype(BF)

    each(0, 4, some(4, make_blocks))

    batch(lbuf, 2 * (Z - 1), L_LEVEL).wait_recv()
    fl[...] = lbuf[...].reshape(Q * 32, 128).astype(F32)
    for tile in range(4):
        rows = [
            fl[pl.ds(s * 8 + n * 4 + tile, Q, stride=32), :] for n in range(2) for s in range(4)
        ]
        block = jnp.concatenate(rows, axis=0)
        lt[:, tile * 128 : (tile + 1) * 128] = block.astype(BF)
        l2[tile * 128 : (tile + 1) * 128, :] = (block.T * (1.0 / S)).astype(BF)

    def outer(t):
        x = dot(l2[...], bd[t]).astype(BF)
        xb[:, 2 * t] = x[:, :128].reshape(Q, C, 128)
        xb[:, 2 * t + 1] = x[:, 128:].reshape(Q, C, 128)

    def grad_w(n):
        total = None
        for p in range(8):
            a = xb[2 * p, pl.ds(n * 8, 8)].reshape(256, 128)
            b = xb[2 * p + 1, pl.ds(n * 8, 8)].reshape(256, 128)
            term = dot(jnp.concatenate([a, b], axis=1), g[p * 256 : (p + 1) * 256, :])
            total = term if total is None else total + term
        gws[pl.ds(pl.multiple_of(n * 256, 256), 256), :] = total

    for t in range(16):
        outer(t)
    for n in range(4):
        grad_w(n)
    def fill_w(m):
        for n in range(4):
            gwsend[m, n] = gws[pl.ds(lax.rem(m, 2) * Q + n * 4 + m // 2, 32, stride=C), :].astype(BF)

    def x_mate(k):
        return lax.rem(me_x + k, 8)

    each(0, 4, some(2, fill_w))
    for k in FAR_FIRST:
        remote(gwsend.at[x_mate(k)], gwx.at[me_x], W_X, (row - me_x + x_mate(k), col)).start()

    def grad_r(t):
        y = jnp.concatenate([yb[:, 2 * t].reshape(512, 128), yb[:, 2 * t + 1].reshape(512, 128)], axis=1)
        x = dot(lt[...], y)
        a, b = x[:S, :128], x[S:, :128]
        c, d = x[:S, 128:], x[S:, 128:]
        grs[t] = jnp.where(low, a, d) + pltpu.roll(jnp.where(low, c, b), 64, 1)

    each(0, 4, some(4, grad_r))

    g_pair = remote(grs.at[:, pl.ds(pl.multiple_of((1 - core) * 32, 32), 32), :], grp, G_PAIR, pair)
    g_pair.start()

    for tile in range(4):
        gls[tile] = jnp.zeros((128, 128), F32)

    def grad_l(n):
        total = None
        for m in range(4):
            t = n * 4 + m
            y = jnp.concatenate(
                [yb[:, 2 * t].reshape(512, 128), yb[:, 2 * t + 1].reshape(512, 128)], axis=1
            )
            term = dot(bd[t], y, ((1,), (1,)))
            total = term if total is None else total + term
        for tile in range(4):
            gls[tile] += total[:, tile * 128 : (tile + 1) * 128]

    each(0, 4, grad_l)

    g_pair.wait_recv()
    grh[...] = (grs[:, pl.ds(pl.multiple_of(core * 32, 32), 32), :] + grp[...]).reshape(512, 128)

    def fill_g(k):
        grsend[chip(k)] = grh[pl.ds(chip(k), 32, stride=Q), :].astype(BF)

    each(0, 4, some(4, fill_g))

    def l_rows(c):
        return jnp.concatenate([gls[tile, pl.ds(c, 8, stride=Q), :] for tile in range(4)], axis=0)

    def fill_l(k):
        for side in range(2):
            glsend[level(k), side] = l_rows(2 * level(k) + side).astype(BF)

    each(0, 2, some(4, fill_l))

    each(1, Z, lambda k: remote(glsend.at[level(k)], glrecv.at[z], L_SUM, z_mate(k)).start())

    batch(gwx, 7, W_X).wait_recv()
    for n in range(4):
        acc = gws[pl.ds(core * Q + n * 4 + me_x // 2, 32, stride=C), :]
        for k in range(1, 8):
            acc = acc + gwx[x_mate(k), n].astype(F32)
        gwysend[n] = acc.astype(BF)

    def y_mate(k):
        there = lax.rem(me_y + k, 8)
        return lax.rem(there, 4), (lax.rem(there, 4) * 8 + me_x, 2 * z + there // 4)

    for k in FAR_FIRST:
        part, mate = y_mate(k)
        remote(gwysend.at[part], gwy.at[me_y], W_Y, mate).start()
    each(1, Q, lambda k: remote(grsend.at[chip(k)], grrecv.at[q], G_ROW, row_mate(k)).start())
    gwy[me_y] = gwysend[lax.rem(me_y, 4)]
    batch(gwy, 7, W_Y).wait_recv()
    acc = gwy[0].astype(F32)
    for n in range(1, 8):
        acc = acc + gwy[n].astype(F32)
    gwzs[...] = acc
    gwz[z] = acc
    for k in FAR_FIRST:
        remote(gwzs, gwz.at[z], W_LEVEL, z_mate(k)).start()

    batch(glrecv, Z - 1, L_SUM).wait_recv()

    def l_total(side):
        acc = l_rows(2 * z + side)
        for k in range(1, Z):
            acc = acc + glrecv[level(k), side].astype(F32)
        return acc

    glys[...] = l_total(1 - yh)
    side_l = remote(glys, gly, L_SUM_SIDE, other)
    side_l.start()
    glf[...] = l_total(yh)

    batch(grrecv, Q - 1, G_ROW).wait_recv()
    acc_r = grh[pl.ds(q, 32, stride=Q), :]
    for k in range(1, Q):
        acc_r = acc_r + grrecv[chip(k)].astype(F32)
    acc_r = acc_r * (1.0 / S)
    grf[0] = acc_r
    grf[1] = pltpu.roll(acc_r, 64, 1)
    for t in range(16):
        for dd in range(2):
            gr_out[2 * t + dd] = grf[dd, 2 * t : 2 * t + 2, :64]

    gt[...] = jnp.zeros_like(gt)
    side_l.wait_recv()
    glf[...] = (glf[...] + gly[...]) * (1.0 / S)
    parts = swap_groups([glf[pl.ds(s, 8, stride=4), :] for s in range(4)], group)
    for a in range(4):
        for tile in range(4):
            gt[tile * 8 + 2 * a : tile * 8 + 2 * a + 2, :] = parts[a][2 * tile : 2 * tile + 2]
    ga[...] = gt[...].T
    for c in range(C):
        gl_out[c] = ga[pl.ds(c % 2 * Q + c // 2, 4, stride=32), :][:, :32]

    batch(gwz, Z - 1, W_LEVEL).wait_recv()
    acc = gwz[0]
    for n in range(1, Z):
        acc = acc + gwz[n]
    gw_out[...] = acc

    batch(r_slots, Q - 1, R_ROW).wait_send()
    l_side.wait_send()
    batch(lbuf, 2 * (Z - 1), L_LEVEL).wait_send()
    r_pair.wait_send()
    batch(gwsend, 7, W_X).wait_send()
    batch(gwy, 7, W_Y).wait_send()
    g_pair.wait_send()
    batch(grsend, Q - 1, G_ROW).wait_send()
    batch(glsend, Z - 1, L_SUM).wait_send()
    side_l.wait_send()
    batch(gwz, Z - 1, W_LEVEL).wait_send()


def put(a_in, b_in, c_in, a_out, b_out, c_out, sem):
    sides = [(a_in, a_out), (b_in, b_out), (c_in, c_out)]
    writes = [pltpu.make_async_copy(src, dst, sem.at[n]) for n, (src, dst) in enumerate(sides)]
    for write in writes:
        write.start()
    for write in writes:
        write.wait()


def body(left_act, right_act, cotangent, weight):
    vm = pltpu.VMEM
    dma = pltpu.SemaphoreType.DMA
    msg = (32, 128)
    parts = pl.pallas_call(
        kernel,
        out_shape=[
            jax.ShapeDtypeStruct(left_act.shape, F32),
            jax.ShapeDtypeStruct(right_act.shape, F32),
            jax.ShapeDtypeStruct(msg, F32),
        ],
        in_specs=[pl.BlockSpec(memory_space=pltpu.HBM)] * 4,
        out_specs=[pl.BlockSpec(memory_space=vm)] * 3,
        scratch_shapes=[
            vm((C, 4, 32), BF), vm((C, 2, 64), BF), vm((2048, 128), BF), vm((1024, 128), BF),
            vm((64, 128), F32), vm((128, 128), F32), vm(msg, F32), vm(msg, BF), vm(msg, BF),
            vm((2, Q, *msg), BF), vm((16, *msg), BF),
            vm((1024, 128), F32), vm((512, 128), F32), vm((1024, 128), F32), vm((1024, 128), BF),
            vm((128, 512), BF), vm((512, 128), BF), vm((16, 128, 256), BF),
            vm((16, C, C, 128), BF), vm((16, C, C, 128), BF),
            vm((1024, 128), F32), vm((8, 4, *msg), BF), vm((8, 4, *msg), BF),
            vm((4, *msg), BF), vm((8, *msg), BF), vm((Z, *msg), F32), vm(msg, F32),
            vm((16, S, 128), F32), vm((16, 32, 128), F32), vm((512, 128), F32),
            vm((Q, *msg), BF), vm((Q, *msg), BF), vm((2, *msg), F32),
            vm((4, 128, 128), F32), vm((Z, 2, *msg), BF), vm((Z, 2, *msg), BF), vm(msg, F32), vm(msg, F32),
            vm(msg, F32), vm((128, 128), F32), vm((128, 128), F32),
            dma((4,)), dma((11,)), dma((11,)),
        ],
        compiler_params=pltpu.CompilerParams(
            collective_id=0, has_side_effects=True, vmem_limit_bytes=32 * 1024 * 1024
        ),
    )(
        *(pltpu.with_memory_space_constraint(a, pltpu.HBM) for a in (left_act, right_act, cotangent.reshape(2048, 128), weight))
    )
    shapes = [part.shape for part in parts]
    return pl.pallas_call(
        put,
        out_shape=[jax.ShapeDtypeStruct(shape, F32) for shape in shapes],
        in_specs=[pl.BlockSpec(memory_space=vm)] * 3,
        out_specs=[pl.BlockSpec(memory_space=pl.ANY)] * 3,
        scratch_shapes=[dma((3,))],
        compiler_params=pltpu.CompilerParams(vmem_limit_bytes=2097152),
    )(*parts)


def solution(mesh):
    return jax.shard_map(
        body,
        mesh=mesh,
        in_specs=(P(None, "col", "row"), P(None, "row", "col"), P("row", "col", None), P()),
        out_specs=(P(None, "col", "row"), P(None, "row", "col"), P("row", None)),
        check_vma=False,
    )
```

```python
import jax
import jax.numpy as jnp
from jax import lax
from jax.experimental import pallas as pl
from jax.experimental.pallas import tpu as pltpu
from jax.sharding import PartitionSpec as P

BF = jnp.bfloat16
F32 = jnp.float32
MESH = pl.DeviceIdType.MESH
S = 64
C = 32
Q = 16
Z = 8
FAR_FIRST = (4, 3, 5, 2, 6, 1, 7)
R_ROW, R_PAIR, L_SIDE, L_LEVEL, W_X, W_Y, W_LEVEL, G_PAIR, G_ROW, L_SUM, L_SUM_SIDE = range(11)


def dot(a, b, dims=((1,), (0,))):
    return lax.dot_general(a, b, (dims, ((), ())), preferred_element_type=F32)


def swap_groups(parts, group):
    outs = []
    for s in range(4):
        out = None
        for a in range(4):
            shift = (a - s) % 4 * 32
            moved = pltpu.roll(parts[a], shift, 1) if shift else parts[a]
            out = moved if out is None else jnp.where(group == a, moved, out)
        outs.append(out)
    return outs


def kernel(
    l_in, r_in, g_in, w_in,
    gl_out, gr_out, gw_out,
    lv, rv, g, w, ra, la, lb, rmsg, lmsg,
    rbuf, lbuf, fr, fl, wf, wp, lt, l2, bd, xb, yb,
    gws, gwsend, gwx, gwysend, gwy, gwz, gwzs,
    grs, grp, grh, grsend, grrecv, grf,
    gls, glsend, glrecv, gly, glys, glf, gt, ga,
    in_sem, sent, got,
):
    row, col = lax.axis_index("row"), lax.axis_index("col")
    core, q = lax.rem(row, 2), row // 2
    yh, z = lax.rem(col, 2), col // 2
    me_x, me_y = lax.rem(row, 8), 4 * yh + row // 8
    pair = (row + 1 - 2 * core, col)
    other = (row, col + 1 - 2 * yh)

    def chip(k):
        return lax.rem(q + k, Q)

    def level(k):
        return lax.rem(z + k, Z)

    def row_mate(k):
        return (2 * chip(k) + core, col)

    def z_mate(k):
        return (row, 2 * level(k) + yh)

    def remote(src, dst, n, device):
        return pltpu.make_async_remote_copy(
            src_ref=src, dst_ref=dst, send_sem=sent.at[n], recv_sem=got.at[n],
            device_id=device, device_id_type=MESH,
        )

    def batch(buf, count, n):
        part = buf.at[pl.ds(0, count)]
        return remote(part, part, n, pair)

    def each(first, last, step):
        def body(k, carry):
            step(k)
            return carry

        lax.fori_loop(first, last, body, 0)

    barrier = pltpu.get_barrier_semaphore()

    def greet(device):
        pl.semaphore_signal(barrier, inc=1, device_id=device, device_id_type=MESH)

    greet(other)
    for k in FAR_FIRST:
        greet(z_mate(k))
    each(1, Q, lambda k: greet(row_mate(k)))
    greet(pair)

    copies = [
        pltpu.make_async_copy(src, dst, in_sem.at[n])
        for n, (src, dst) in enumerate([(r_in, rv), (l_in, lv), (w_in, w), (g_in, g)])
    ]
    for copy in copies:
        copy.start()

    lane = lax.broadcasted_iota(jnp.int32, (S, 128), 1)
    low = lane < 64
    group = lane[:8] // 32

    ra[...] = jnp.zeros_like(ra)
    la[...] = jnp.zeros_like(la)
    copies[0].wait()
    for d in range(C):
        ra[2 * d : 2 * d + 2, :64] = rv[d].astype(F32)
    for s in range(2):
        a = ra[pl.ds(s, 16, stride=4), :]
        b = ra[pl.ds(2 + s, 16, stride=4), :]
        rmsg[s * 16 : s * 16 + 16, :] = jnp.where(low[:16], a, pltpu.roll(b, 64, 1)).astype(BF)

    copies[1].wait()
    for c in range(C):
        la[4 * c : 4 * c + 4, :32] = lv[c].astype(F32)
    stack = [la[pl.ds(half * 4 + s, Q, stride=8), :] for s in range(4) for half in range(2)]
    lb[...] = jnp.concatenate(stack, axis=0).T[:32]
    parts = [
        jnp.concatenate([lb[pl.ds(2 * a + n, 4, stride=8), :] for n in range(2)], axis=0)
        for a in range(4)
    ]
    lmsg[...] = jnp.concatenate(swap_groups(parts, group), axis=0).astype(BF)
    rbuf[core, q] = rmsg[...]
    lbuf[col] = lmsg[...]

    pl.semaphore_wait(barrier, Q + Z)

    side_col = col + 1 - 2 * yh
    l_side = remote(lmsg, lbuf.at[col], L_SIDE, other)
    l_side.start()
    r_slots = rbuf.at[core]
    each(1, Q, lambda k: remote(rmsg, r_slots.at[q], R_ROW, row_mate(k)).start())
    for k in FAR_FIRST:
        remote(lmsg, lbuf.at[col], L_LEVEL, z_mate(k)).start()

    copies[2].wait()
    wf[...] = w[...].astype(F32)

    def order_weight(d):
        for half in range(2):
            rows = wf[pl.ds(half * C + d, Q, stride=2 * C), :]
            wp[pl.ds(pl.multiple_of(d * C + half * Q, Q), Q), :] = rows.astype(BF)

    def some(count, step):
        def body(n):
            for m in range(count):
                step(n * count + m)

        return body

    each(0, C // 8, some(8, order_weight))
    copies[3].wait()

    def grad_outer(p):
        gp = g[pl.ds(pl.multiple_of(p * 256, 256), 256), :]
        y = dot(wp[...], gp, ((1,), (1,))).astype(BF)
        yb[2 * p] = y[:, :128].reshape(C, C, 128)
        yb[2 * p + 1] = y[:, 128:].reshape(C, C, 128)

    each(0, 8, grad_outer)

    l_side.wait_recv()
    forward = lbuf.at[side_col]
    for k in FAR_FIRST:
        remote(forward, forward, L_LEVEL, z_mate(k)).start()

    batch(r_slots, Q - 1, R_ROW).wait_recv()
    r_pair = remote(r_slots, r_slots, R_PAIR, pair)
    r_pair.start()

    r_pair.wait_recv()
    fr[...] = rbuf[...].reshape(2 * Q * 32, 128).astype(F32)

    def make_blocks(t):
        rows = [
            fr[pl.ds(half * 512 + s * 16 + t, Q, stride=32), :] for half in range(2) for s in range(2)
        ]
        v = jnp.concatenate(rows, axis=0)
        u = pltpu.roll(v, 64, 1)
        zero = jnp.zeros_like(v)
        bd[t, :S, :128] = jnp.where(low, v, zero).astype(BF)
        bd[t, :S, 128:] = jnp.where(low, u, zero).astype(BF)
        bd[t, S:, :128] = jnp.where(low, zero, u).astype(BF)
        bd[t, S:, 128:] = jnp.where(low, zero, v).astype(BF)

    each(0, 4, some(4, make_blocks))

    batch(lbuf, 2 * (Z - 1), L_LEVEL).wait_recv()
    fl[...] = lbuf[...].reshape(Q * 32, 128).astype(F32)
    for tile in range(4):
        rows = [
            fl[pl.ds(s * 8 + n * 4 + tile, Q, stride=32), :] for n in range(2) for s in range(4)
        ]
        block = jnp.concatenate(rows, axis=0)
        lt[:, tile * 128 : (tile + 1) * 128] = block.astype(BF)
        l2[tile * 128 : (tile + 1) * 128, :] = (block.T * (1.0 / S)).astype(BF)

    def outer(t):
        x = dot(l2[...], bd[t]).astype(BF)
        xb[:, 2 * t] = x[:, :128].reshape(Q, C, 128)
        xb[:, 2 * t + 1] = x[:, 128:].reshape(Q, C, 128)

    def grad_w(n):
        total = None
        for p in range(8):
            a = xb[2 * p, pl.ds(n * 8, 8)].reshape(256, 128)
            b = xb[2 * p + 1, pl.ds(n * 8, 8)].reshape(256, 128)
            term = dot(jnp.concatenate([a, b], axis=1), g[p * 256 : (p + 1) * 256, :])
            total = term if total is None else total + term
        gws[pl.ds(pl.multiple_of(n * 256, 256), 256), :] = total

    for t in range(16):
        outer(t)
    for n in range(4):
        grad_w(n)
    def fill_w(m):
        for n in range(4):
            gwsend[m, n] = gws[pl.ds(lax.rem(m, 2) * Q + n * 4 + m // 2, 32, stride=C), :].astype(BF)

    def x_mate(k):
        return lax.rem(me_x + k, 8)

    each(0, 4, some(2, fill_w))
    for k in FAR_FIRST:
        remote(gwsend.at[x_mate(k)], gwx.at[me_x], W_X, (row - me_x + x_mate(k), col)).start()

    def grad_r(t):
        y = jnp.concatenate([yb[:, 2 * t].reshape(512, 128), yb[:, 2 * t + 1].reshape(512, 128)], axis=1)
        x = dot(lt[...], y)
        a, b = x[:S, :128], x[S:, :128]
        c, d = x[:S, 128:], x[S:, 128:]
        grs[t] = jnp.where(low, a, d) + pltpu.roll(jnp.where(low, c, b), 64, 1)

    each(0, 4, some(4, grad_r))

    g_pair = remote(grs.at[:, pl.ds(pl.multiple_of((1 - core) * 32, 32), 32), :], grp, G_PAIR, pair)
    g_pair.start()

    for tile in range(4):
        gls[tile] = jnp.zeros((128, 128), F32)

    def grad_l(n):
        total = None
        for m in range(4):
            t = n * 4 + m
            y = jnp.concatenate(
                [yb[:, 2 * t].reshape(512, 128), yb[:, 2 * t + 1].reshape(512, 128)], axis=1
            )
            term = dot(bd[t], y, ((1,), (1,)))
            total = term if total is None else total + term
        for tile in range(4):
            gls[tile] += total[:, tile * 128 : (tile + 1) * 128]

    each(0, 4, grad_l)

    g_pair.wait_recv()
    grh[...] = (grs[:, pl.ds(pl.multiple_of(core * 32, 32), 32), :] + grp[...]).reshape(512, 128)

    def fill_g(k):
        grsend[chip(k)] = grh[pl.ds(chip(k), 32, stride=Q), :].astype(BF)

    each(0, 4, some(4, fill_g))

    def l_rows(c):
        return jnp.concatenate([gls[tile, pl.ds(c, 8, stride=Q), :] for tile in range(4)], axis=0)

    def fill_l(k):
        for side in range(2):
            glsend[level(k), side] = l_rows(2 * level(k) + side).astype(BF)

    each(0, 2, some(4, fill_l))

    for k in FAR_FIRST:
        remote(glsend.at[level(k)], glrecv.at[z], L_SUM, z_mate(k)).start()

    batch(gwx, 7, W_X).wait_recv()
    for n in range(4):
        acc = gws[pl.ds(core * Q + n * 4 + me_x // 2, 32, stride=C), :]
        for k in range(1, 8):
            acc = acc + gwx[x_mate(k), n].astype(F32)
        gwysend[n] = acc.astype(BF)

    def y_mate(k):
        there = lax.rem(me_y + k, 8)
        return lax.rem(there, 4), (lax.rem(there, 4) * 8 + me_x, 2 * z + there // 4)

    for k in FAR_FIRST:
        part, mate = y_mate(k)
        remote(gwysend.at[part], gwy.at[me_y], W_Y, mate).start()
    each(1, Q, lambda k: remote(grsend.at[chip(k)], grrecv.at[q], G_ROW, row_mate(k)).start())
    gwy[me_y] = gwysend[lax.rem(me_y, 4)]
    batch(gwy, 7, W_Y).wait_recv()
    acc = gwy[0].astype(F32)
    for n in range(1, 8):
        acc = acc + gwy[n].astype(F32)
    gwzs[...] = acc
    gwz[z] = acc
    for k in FAR_FIRST:
        remote(gwzs, gwz.at[z], W_LEVEL, z_mate(k)).start()

    batch(glrecv, Z - 1, L_SUM).wait_recv()

    def l_total(side):
        acc = l_rows(2 * z + side)
        for k in range(1, Z):
            acc = acc + glrecv[level(k), side].astype(F32)
        return acc

    glys[...] = l_total(1 - yh)
    side_l = remote(glys, gly, L_SUM_SIDE, other)
    side_l.start()
    glf[...] = l_total(yh)

    batch(grrecv, Q - 1, G_ROW).wait_recv()
    acc_r = grh[pl.ds(q, 32, stride=Q), :]
    for k in range(1, Q):
        acc_r = acc_r + grrecv[chip(k)].astype(F32)
    acc_r = acc_r * (1.0 / S)
    grf[0] = acc_r
    grf[1] = pltpu.roll(acc_r, 64, 1)
    for t in range(16):
        for dd in range(2):
            gr_out[2 * t + dd] = grf[dd, 2 * t : 2 * t + 2, :64]

    gt[...] = jnp.zeros_like(gt)
    side_l.wait_recv()
    glf[...] = (glf[...] + gly[...]) * (1.0 / S)
    parts = swap_groups([glf[pl.ds(s, 8, stride=4), :] for s in range(4)], group)
    for a in range(4):
        for tile in range(4):
            gt[tile * 8 + 2 * a : tile * 8 + 2 * a + 2, :] = parts[a][2 * tile : 2 * tile + 2]
    ga[...] = gt[...].T
    for c in range(C):
        gl_out[c] = ga[pl.ds(c % 2 * Q + c // 2, 4, stride=32), :][:, :32]

    batch(gwz, Z - 1, W_LEVEL).wait_recv()
    acc = gwz[0]
    for n in range(1, Z):
        acc = acc + gwz[n]
    gw_out[...] = acc

    batch(r_slots, Q - 1, R_ROW).wait_send()
    l_side.wait_send()
    batch(lbuf, 2 * (Z - 1), L_LEVEL).wait_send()
    r_pair.wait_send()
    batch(gwsend, 7, W_X).wait_send()
    batch(gwy, 7, W_Y).wait_send()
    g_pair.wait_send()
    batch(grsend, Q - 1, G_ROW).wait_send()
    batch(glsend, Z - 1, L_SUM).wait_send()
    side_l.wait_send()
    batch(gwz, Z - 1, W_LEVEL).wait_send()


def put(a_in, b_in, c_in, a_out, b_out, c_out, sem):
    sides = [(a_in, a_out), (b_in, b_out), (c_in, c_out)]
    writes = [pltpu.make_async_copy(src, dst, sem.at[n]) for n, (src, dst) in enumerate(sides)]
    for write in writes:
        write.start()
    for write in writes:
        write.wait()


def body(left_act, right_act, cotangent, weight):
    vm = pltpu.VMEM
    dma = pltpu.SemaphoreType.DMA
    msg = (32, 128)
    parts = pl.pallas_call(
        kernel,
        out_shape=[
            jax.ShapeDtypeStruct(left_act.shape, F32),
            jax.ShapeDtypeStruct(right_act.shape, F32),
            jax.ShapeDtypeStruct(msg, F32),
        ],
        in_specs=[pl.BlockSpec(memory_space=pltpu.HBM)] * 4,
        out_specs=[pl.BlockSpec(memory_space=vm)] * 3,
        scratch_shapes=[
            vm((C, 4, 32), BF), vm((C, 2, 64), BF), vm((2048, 128), BF), vm((1024, 128), BF),
            vm((64, 128), F32), vm((128, 128), F32), vm(msg, F32), vm(msg, BF), vm(msg, BF),
            vm((2, Q, *msg), BF), vm((16, *msg), BF),
            vm((1024, 128), F32), vm((512, 128), F32), vm((1024, 128), F32), vm((1024, 128), BF),
            vm((128, 512), BF), vm((512, 128), BF), vm((16, 128, 256), BF),
            vm((16, C, C, 128), BF), vm((16, C, C, 128), BF),
            vm((1024, 128), F32), vm((8, 4, *msg), BF), vm((8, 4, *msg), BF),
            vm((4, *msg), BF), vm((8, *msg), BF), vm((Z, *msg), F32), vm(msg, F32),
            vm((16, S, 128), F32), vm((16, 32, 128), F32), vm((512, 128), F32),
            vm((Q, *msg), BF), vm((Q, *msg), BF), vm((2, *msg), F32),
            vm((4, 128, 128), F32), vm((Z, 2, *msg), BF), vm((Z, 2, *msg), BF), vm(msg, F32), vm(msg, F32),
            vm(msg, F32), vm((128, 128), F32), vm((128, 128), F32),
            dma((4,)), dma((11,)), dma((11,)),
        ],
        compiler_params=pltpu.CompilerParams(
            collective_id=0, has_side_effects=True, vmem_limit_bytes=32 * 1024 * 1024
        ),
    )(
        *(pltpu.with_memory_space_constraint(a, pltpu.HBM) for a in (left_act, right_act, cotangent.reshape(2048, 128), weight))
    )
    shapes = [part.shape for part in parts]
    return pl.pallas_call(
        put,
        out_shape=[jax.ShapeDtypeStruct(shape, F32) for shape in shapes],
        in_specs=[pl.BlockSpec(memory_space=vm)] * 3,
        out_specs=[pl.BlockSpec(memory_space=pl.ANY)] * 3,
        scratch_shapes=[dma((3,))],
        compiler_params=pltpu.CompilerParams(vmem_limit_bytes=2097152),
    )(*parts)


def solution(mesh):
    return jax.shard_map(
        body,
        mesh=mesh,
        in_specs=(P(None, "col", "row"), P(None, "row", "col"), P("row", "col", None), P()),
        out_specs=(P(None, "col", "row"), P(None, "row", "col"), P("row", None)),
        check_vma=False,
    )
```
